32 devices in a mesh: aa: 8 (over z, x), ba: 4 (over y, core).
Axes of the slice: x: 2, y: 2, z: 4, core: 2. Of those that a mesh axis runs over, the one named last changes fastest.
Arguments:
- residual_a: bfloat16 [64, 4096], P('ba', 'aa'), may hold values from -160 to 160
- residual_b: bfloat16 [64, 3584], P(('aa', 'ba')), may hold values from -160 to 160
- encoder_a: bfloat16 [4096, 16384], P('ba', 'aa'), may hold values from -1 to 1
- bias_a: float32 [16384], P('aa'), may hold values from -12 to 12
- encoder_b: bfloat16 [3584, 16384], P('aa', 'ba'), may hold values from -1 to 1
- bias_b: float32 [16384], P('ba'), may hold values from -12 to 12
Outputs:
- match_score: float32 [16384, 16384], P('aa', 'ba')
- row_level: float32 [16384], P('aa')
- column_level: float32 [16384], P('ba')
The draws below stay inside these ranges and needn't reach their ends.
All inputs are finite; a program needn't handle non-finite values.
Results may differ from the reference program's by a relative error of at most 0.0004.
The reference program's roundings to bfloat16 on the way (of `unit_a` and `unit_b`) count: a program that leaves them out, or rounds other values in their place, can miss the bound.
Values may be sent and summed in bfloat16 or wider, within the bound.
No kernel may reach another device: no remote copies, remote signals or barrier semaphores. Data moves between devices by JAX's collectives and lax.ppermute only.
A program may use at most 128 MiB of HBM per device.

```python
import math
import jax
import jax.numpy as jnp
from jax import lax

DA = 4096
DB = 3584
FA = 16384
FB = 16384
INV_TEMP = 256
TOKENS = 64


def draw_residual_a(key, part):
    key_list = jax.random.split(jax.random.fold_in(key, 11), 2)
    position = jnp.arange(TOKENS, dtype=jnp.float32) / TOKENS
    scales = jnp.exp(jax.random.uniform(key_list[0], (TOKENS,), jnp.float32, 0.0, math.log(10.0))) * jnp.exp(position * math.log(3.0))
    noise_part = jnp.clip(jax.random.normal(key_list[1], (TOKENS, DA), jnp.float32), -5.0, 5.0)
    values = jnp.clip(scales[:, None] * noise_part, -160.0, 160.0)
    return values.astype(jnp.bfloat16)


def draw_residual_b(key, part):
    key_list = jax.random.split(jax.random.fold_in(key, 12), 2)
    position = jnp.arange(TOKENS, dtype=jnp.float32) / TOKENS
    scales = jnp.exp(jax.random.uniform(key_list[0], (TOKENS,), jnp.float32, 0.0, math.log(10.0))) * jnp.exp(position * math.log(3.0))
    noise_part = jnp.clip(jax.random.normal(key_list[1], (TOKENS, DB), jnp.float32), -5.0, 5.0)
    values = jnp.clip(scales[:, None] * noise_part, -160.0, 160.0)
    return values.astype(jnp.bfloat16)


def draw_encoder_a(key, part):
    seed_key = jax.random.fold_in(key, 21)
    weights = jnp.clip(jax.random.normal(seed_key, (DA, FA), jnp.float32), -5.0, 5.0) / math.sqrt(DA)
    return weights.astype(jnp.bfloat16)


def draw_encoder_b(key, part):
    seed_key = jax.random.fold_in(key, 22)
    weights = jnp.clip(jax.random.normal(seed_key, (DB, FB), jnp.float32), -5.0, 5.0) / math.sqrt(DB)
    return weights.astype(jnp.bfloat16)


def block_scale(own_key, shape, cuts, least, largest):
    def one(dim, shards_of):
        steps = jax.random.uniform(jax.random.fold_in(jax.random.fold_in(own_key, 6), dim), (shards_of,), jnp.float32, least / len(cuts), largest / len(cuts))
        return jnp.repeat(jnp.exp(steps), shape[dim] // shards_of).reshape((-1,) + (1,) * (len(shape) - dim - 1))

    level = one(*cuts[0])
    for cut in cuts[1:]:
        level = level * one(*cut)
    return level


def noise(own_key, extent, deviation, most, shards=(), kind=jnp.bfloat16):
    factor_of = block_scale(own_key, extent, shards, -0.22, 0.18) if shards else 1.0
    result = jax.random.normal(own_key, extent, jnp.float32) * deviation * factor_of
    return jnp.minimum(jnp.maximum(result, -most), most).astype(kind)


def setup_inputs(seed: int = 0) -> dict:
    key_of = jax.random.split(jax.random.key(seed), 7)
    return {
        "residual_a": draw_residual_a(jax.random.fold_in(key_of[6], 71), 0),
        "residual_b": draw_residual_b(jax.random.fold_in(key_of[6], 71), 0),
        "encoder_a": draw_encoder_a(jax.random.fold_in(key_of[6], 71), 0),
        "bias_a": noise(key_of[3], (FA,), 2.0, 12.0, ((0, 8),), jnp.float32),
        "encoder_b": draw_encoder_b(jax.random.fold_in(key_of[6], 71), 0),
        "bias_b": noise(key_of[5], (FB,), 2.0, 12.0, ((0, 4),), jnp.float32),
    }


epsilon = 1e-05

def standardize(fired):
    mean_part = lax.optimization_barrier(jnp.mean(fired, axis=0))
    centered = fired - mean_part[None, :]
    spread = lax.optimization_barrier(jnp.mean(centered * centered, axis=0))
    return (centered * lax.rsqrt(spread + epsilon)[None, :]).astype(jnp.bfloat16)

def reference(residual_a, residual_b, encoder_a, bias_a, encoder_b, bias_b):
    token_total = residual_a.shape[0]
    fired_a = jnp.maximum(jnp.dot(residual_a, encoder_a, preferred_element_type=jnp.float32) + bias_a[None, :], 0.0)
    fired_b = jnp.maximum(jnp.dot(residual_b, encoder_b, preferred_element_type=jnp.float32) + bias_b[None, :], 0.0)
    unit_a = standardize(fired_a)
    unit_b = standardize(fired_b)
    correlation = jnp.dot(unit_a.T, unit_b, preferred_element_type=jnp.float32) / token_total
    scores = correlation * INV_TEMP
    row_top = lax.optimization_barrier(jnp.max(scores, axis=1))
    row_level = (row_top + jnp.log(lax.optimization_barrier(jnp.sum(jnp.exp(scores - row_top[:, None]), axis=1)))) / INV_TEMP
    column_top = lax.optimization_barrier(jnp.max(scores, axis=0))
    column_level = (column_top + jnp.log(lax.optimization_barrier(jnp.sum(jnp.exp(scores - column_top[None, :]), axis=0)))) / INV_TEMP
    match_score = correlation - 0.5 * (row_level[:, None] + column_level[None, :])
    return (match_score, row_level, column_level)
```

```python
import functools
import math

import jax
import jax.numpy as jnp
from jax import lax
from jax.experimental import pallas as pl
from jax.experimental.pallas import tpu as pltpu
from jax.sharding import PartitionSpec as P

INV_TEMP = 256
LOG2E = math.log2(math.e)
LANES = 128

epsilon = 1e-05


def tile(size, most):
    while size % most:
        most //= 2
    return most


def transpose_into(source, target):
    for k in range(source.shape[1] // LANES):
        part = slice(k * LANES, (k + 1) * LANES)
        target[part, :] = source[:, part].T


def stats_kernel(scale, a_ref, b_ref, row_ref, column_ref, at, row_top, row_sum, column_top, column_sum):
    rows = a_ref.shape[1]
    blocks, _, width = b_ref.shape
    tall = tile(rows, 256)
    low = jnp.finfo(jnp.float32).min
    transpose_into(a_ref, at)
    row_top[...] = jnp.full_like(row_top, low)
    column_top[...] = jnp.full_like(column_top, low)
    row_sum[...] = jnp.zeros_like(row_sum)
    column_sum[...] = jnp.zeros_like(column_sum)

    def scaled(r, block):
        dots = jnp.dot(at[pl.ds(r, tall), :], b_ref[block], preferred_element_type=jnp.float32)
        return dots * scale

    def lanes_of(values, combine):
        total = values[:, :LANES]
        for k in range(1, width // LANES):
            total = combine(total, values[:, k * LANES : (k + 1) * LANES])
        return total

    def sublanes_of(values, combine):
        total = values[:8]
        for k in range(1, tall // 8):
            total = combine(total, values[k * 8 : (k + 1) * 8])
        return total

    def walk(step):
        def over_blocks(block, carry):
            def over_rows(k, carry):
                step(pl.multiple_of(k * tall, tall), block)
                return carry

            return lax.fori_loop(0, rows // tall, over_rows, carry)

        lax.fori_loop(0, blocks, over_blocks, 0)

    def top_step(r, block):
        x = scaled(r, block)
        here = pl.ds(r, tall)
        row_top[here, :] = jnp.maximum(row_top[here, :], lanes_of(x, jnp.maximum))
        column_top[block] = jnp.maximum(column_top[block], sublanes_of(x, jnp.maximum))

    walk(top_step)
    for k in range(rows // LANES):
        part = slice(k * LANES, (k + 1) * LANES)
        top = jnp.max(row_top[part, :], axis=1, keepdims=True)
        row_top[part, :] = jnp.broadcast_to(top, (LANES, LANES))
    for k in range(blocks):
        top = jnp.max(column_top[k], axis=0, keepdims=True)
        column_top[k] = jnp.broadcast_to(top, (8, width))

    def sum_step(r, block):
        x = scaled(r, block)
        here = pl.ds(r, tall)
        top = row_top[here, :]
        by_row = jnp.exp2(x - jnp.concatenate([top] * (width // LANES), axis=1))
        row_sum[here, :] = row_sum[here, :] + lanes_of(by_row, jnp.add)
        by_column = jnp.exp2(x - jnp.broadcast_to(column_top[block, :1], (tall, width)))
        column_sum[block] = column_sum[block] + sublanes_of(by_column, jnp.add)

    walk(sum_step)
    for k in range(rows // LANES):
        part = slice(k * LANES, (k + 1) * LANES)
        mass = jnp.sum(row_sum[part, :].T, axis=0, keepdims=True)
        row_ref[:, part] = row_top[part, :].T[:1] + jnp.log2(mass)
    for k in range(blocks):
        mass = jnp.sum(column_sum[k], axis=0, keepdims=True)
        column_ref[k] = column_top[k, :1] + jnp.log2(mass)


def stats(a, b, scale):
    tokens, rows = a.shape
    blocks, _, width = b.shape
    elements = rows * blocks * width
    return pl.pallas_call(
        functools.partial(stats_kernel, scale),
        out_shape=(
            jax.ShapeDtypeStruct((1, rows), jnp.float32),
            jax.ShapeDtypeStruct((blocks, 1, width), jnp.float32),
        ),
        in_specs=[pl.BlockSpec(memory_space=pltpu.VMEM)] * 2,
        out_specs=[pl.BlockSpec(memory_space=pltpu.VMEM)] * 2,
        scratch_shapes=[
            pltpu.VMEM((rows, tokens), jnp.bfloat16),
            pltpu.VMEM((rows, LANES), jnp.float32),
            pltpu.VMEM((rows, LANES), jnp.float32),
            pltpu.VMEM((blocks, 8, width), jnp.float32),
            pltpu.VMEM((blocks, 8, width), jnp.float32),
        ],
        cost_estimate=pl.CostEstimate(flops=4 * elements * tokens, bytes_accessed=0, transcendentals=2 * elements),
        name="stats",
    )(a, b)


def match_kernel(share, a_ref, b_ref, row_ref, column_ref, out_ref, at, half):
    tall = out_ref.shape[0]
    blocks, _, width = b_ref.shape

    @pl.when(pl.program_id(0) == 0)
    def _():
        transpose_into(a_ref, at)
        for k in range(at.shape[0] // LANES):
            part = slice(k * LANES, (k + 1) * LANES)
            half[part, :] = jnp.broadcast_to(row_ref[:, part] * 0.5, (LANES, LANES)).T

    r = pl.multiple_of(pl.program_id(0) * tall, tall)
    here = pl.ds(r, tall)
    row_half = jnp.concatenate([half[here, :]] * (width // LANES), axis=1)
    for block in range(blocks):
        dots = jnp.dot(at[here, :], b_ref[block], preferred_element_type=jnp.float32)
        column_half = jnp.broadcast_to(column_ref[block] * 0.5, (tall, width))
        out_ref[:, block * width : (block + 1) * width] = dots * share - (row_half + column_half)


def match(a, b, row_level, column_level, share):
    tokens, rows = a.shape
    blocks, _, width = b.shape
    tall = tile(rows, 256)
    return pl.pallas_call(
        functools.partial(match_kernel, share),
        grid=(rows // tall,),
        out_shape=jax.ShapeDtypeStruct((rows, blocks * width), jnp.float32),
        in_specs=[pl.BlockSpec(memory_space=pltpu.VMEM)] * 4,
        out_specs=pl.BlockSpec((tall, blocks * width), lambda r: (r, 0)),
        scratch_shapes=[
            pltpu.VMEM((rows, tokens), jnp.bfloat16),
            pltpu.VMEM((rows, LANES), jnp.float32),
        ],
        cost_estimate=pl.CostEstimate(
            flops=2 * rows * blocks * width * tokens, bytes_accessed=4 * rows * blocks * width, transcendentals=0
        ),
        name="match",
    )(a, b, row_level, column_level)


def swap(value, axis, distance):
    size = lax.axis_size(axis)
    return lax.ppermute(value, axis, [(k, k ^ distance) for k in range(size)])


def pieces_of(value, axis):
    size = lax.axis_size(axis)
    me = lax.axis_index(axis)
    width = value.shape[1] // size
    return [lax.dynamic_slice_in_dim(value, (me ^ d) * width, width, axis=1) for d in range(size)]


def scatter_sum(value, axis):
    size = lax.axis_size(axis)
    pieces = pieces_of(value, axis)
    total = pieces[0]
    for part in [swap(pieces[d], axis, d) for d in range(size - 1, 0, -1)]:
        total = total + part
    return total


def staged_scatter_sum(value, axis):
    size = lax.axis_size(axis)
    if size < 4:
        return scatter_sum(value, axis)
    pieces = pieces_of(value, axis)
    keep = jnp.concatenate(pieces[0::2], axis=1)
    keep = keep + swap(jnp.concatenate(pieces[1::2], axis=1), axis, 1)
    parts = jnp.split(keep, size // 2, axis=1)
    total = parts[0]
    for part in [swap(parts[d // 2], axis, d) for d in range(size - 2, 0, -2)]:
        total = total + part
    return total


def everyone(value, axis):
    size = lax.axis_size(axis)
    return lax.all_to_all(jnp.broadcast_to(value[None], (size,) + value.shape), axis, 0, 0, tiled=True)


def standardize(encoded, bias, axis):
    width = encoded.shape[1]
    bias = lax.dynamic_slice_in_dim(bias, lax.axis_index(axis) * width, width)
    fired = jnp.maximum(encoded + bias[None, :], 0.0)
    centered = fired - jnp.mean(fired, axis=0)[None, :]
    spread = jnp.mean(centered * centered, axis=0)
    return (centered * lax.rsqrt(spread + epsilon)[None, :]).astype(jnp.bfloat16)


def level(parts):
    top = jnp.max(parts, axis=0)
    return (top + jnp.log2(jnp.sum(jnp.exp2(parts - top[None]), axis=0))) * (1.0 / (LOG2E * INV_TEMP))


def per_device(residual_a, residual_b, encoder_a, bias_a, encoder_b, bias_b):
    size_a, size_b = lax.axis_size("aa"), lax.axis_size("ba")
    index_a = lax.axis_index("aa")
    both = ("aa", "ba")

    ratio = size_a // size_b
    assert ratio * size_b == size_a
    tokens_a = lax.all_gather(residual_a, "ba", axis=0, tiled=True)
    tokens = tokens_a.shape[0]
    got = []
    for p in range(ratio):
        pairs = [
            ((ratio * j + (i + p) % ratio) * size_b + i // ratio, i * size_b + j)
            for i in range(size_a)
            for j in range(size_b)
        ]
        got.append(lax.ppermute(tokens_a, both, pairs))
    columns_a = jnp.stack(got)
    columns_a = jnp.roll(columns_a, index_a % ratio, axis=0)
    columns_a = jnp.transpose(columns_a, (1, 0, 2)).reshape(tokens, -1)

    own, depth = residual_b.shape[0], residual_b.shape[1] // size_a
    slabs = jnp.transpose(residual_b.reshape(own, size_a, depth), (1, 0, 2))
    slabs = jnp.broadcast_to(slabs[:, None], (size_a, size_b, own, depth)).reshape(-1, own, depth)
    columns_b = lax.all_to_all(slabs, both, 0, 0, tiled=True).reshape(tokens, depth)

    partial_b = jnp.dot(columns_b, encoder_b, preferred_element_type=jnp.float32)
    encoded_b = staged_scatter_sum(partial_b, "aa")
    partial_a = jnp.dot(columns_a, encoder_a, preferred_element_type=jnp.float32)
    encoded_a = scatter_sum(partial_a, "ba")

    unit_a = standardize(encoded_a, bias_a, "ba")
    every_a = lax.all_gather(unit_a, "ba", axis=1, tiled=True)
    unit_b = standardize(encoded_b, bias_b, "aa")
    every_b = everyone(unit_b, "aa")

    if every_b.shape[2] % LANES:
        every_b = jnp.transpose(every_b, (1, 0, 2)).reshape(1, tokens, -1)
    row_part, column_part = stats(every_a, every_b, LOG2E * INV_TEMP / tokens)
    row_parts = jnp.stack([row_part] + [swap(row_part, "ba", d) for d in range(size_b - 1, 0, -1)])
    row_level = level(row_parts)
    column_level = level(everyone(column_part, "aa"))
    match_score = match(every_a, every_b, row_level, column_level, 1.0 / tokens)
    return (match_score, row_level.reshape(-1), column_level.reshape(-1))


def solution(mesh):
    return jax.shard_map(
        per_device,
        mesh=mesh,
        in_specs=(
            P("ba", "aa"),
            P(("aa", "ba"), None),
            P("ba", "aa"),
            P("aa"),
            P("aa", "ba"),
            P("ba"),
        ),
        out_specs=(P("aa", "ba"), P("aa"), P("ba")),
        check_vma=False,
    )
```

```python
import functools
import math

import jax
import jax.numpy as jnp
from jax import lax
from jax.experimental import pallas as pl
from jax.experimental.pallas import tpu as pltpu
from jax.sharding import PartitionSpec as P


INV_TEMP = 256
LOG2E = math.log2(math.e)
LANES = 128

NEAR_B = 4

epsilon = 1e-05


HIGH, LOW = 260.0, 52.0
FLOOR = 2.0**-96


def tile(size, most):
    while size % most:
        most //= 2
    return most


def round_up(size, unit):
    return -(-size // unit) * unit


def lanes_of(values, combine):
    total = values[:, :LANES]
    for k in range(1, values.shape[1] // LANES):
        total = combine(total, values[:, k * LANES : (k + 1) * LANES])
    return total


def sublanes_of(values, combine):
    total = values[:8]
    for k in range(1, values.shape[0] // 8):
        total = combine(total, values[k * 8 : (k + 1) * 8])
    return total


def three(value):
    high = value.astype(jnp.bfloat16)
    rest = value - high.astype(jnp.float32)
    middle = rest.astype(jnp.bfloat16)
    low = (rest - middle.astype(jnp.float32)).astype(jnp.bfloat16)
    return [high, middle, low]


def stats_kernel(scale, place_a, place_b, moved, *refs):
    a_parts, refs = refs[: len(place_a)], refs[len(place_a) :]
    b_parts, refs = refs[: len(place_b)], refs[len(place_b) :]
    row_ref, column_ref, a_all, b_all, at, bt, row_one, row_two, column_one, column_two = refs
    tokens, rows = a_all.shape
    columns = b_all.shape[1]
    part_a, part_b = row_ref.shape[1], column_ref.shape[1]
    depth = at.shape[1]
    used = 3 * tokens
    index = [lax.axis_index("aa"), lax.axis_index("ba")] if moved else [0, 0]

    spot = lax.broadcasted_iota(jnp.int32, (rows, depth - used), 1) == 0
    at[:, used:] = jnp.where(spot, -HIGH, 0.0).astype(jnp.bfloat16)
    spot = lax.broadcasted_iota(jnp.int32, (depth - used, columns), 0) == 0
    bt[used:, :] = jnp.where(spot, 1.0, 0.0).astype(jnp.bfloat16)
    for part, places in zip(a_parts, place_a):
        for q, place in enumerate(places):
            first = lax.bitwise_xor(index[1], place) * part_a
            block = part[:, q * part_a : (q + 1) * part_a]
            a_all[:, pl.ds(pl.multiple_of(first, part_a), part_a)] = block
            terms = jnp.concatenate(three(block.astype(jnp.float32) * scale), axis=0)
            for k in range(part_a // LANES):
                here = pl.ds(pl.multiple_of(first + k * LANES, LANES), LANES)
                at[here, :used] = terms[:, k * LANES : (k + 1) * LANES].T
    for part, places in zip(b_parts, place_b):
        for q, place in enumerate(places):
            block = part[:, q * part_b : (q + 1) * part_b]
            here = pl.ds(pl.multiple_of(lax.bitwise_xor(index[0], place) * part_b, part_b), part_b)
            b_all[:, here] = block
            for k in range(3):
                bt[k * tokens : (k + 1) * tokens, here] = block

    wide = tile(columns, 512)
    tall = tile(rows, 512)
    row_one[...] = jnp.zeros_like(row_one)
    row_two[...] = jnp.zeros_like(row_two)

    def over_columns(c, carry):
        here = pl.ds(pl.multiple_of(c * wide, wide), wide)
        one = jnp.zeros((8, wide), jnp.float32)
        two = one
        for k in range(rows // tall):
            band = slice(k * tall, (k + 1) * tall)
            x = jnp.dot(at[band, :], bt[:, here], preferred_element_type=jnp.float32)
            e = jnp.exp2(x)
            row_one[band, :] = row_one[band, :] + lanes_of(e, jnp.add)
            one = one + sublanes_of(e, jnp.add)
            e = jnp.exp2(x + (HIGH - LOW))
            row_two[band, :] = row_two[band, :] + lanes_of(e, jnp.add)
            two = two + sublanes_of(e, jnp.add)
        column_one[:, here] = one
        column_two[:, here] = two
        return carry

    lax.fori_loop(0, columns // wide, over_columns, 0)

    worst = jnp.full((1, LANES), jnp.inf, jnp.float32)

    def pick(one, two):
        return jnp.where(one >= FLOOR, jnp.log2(one) + HIGH, jnp.log2(two) + LOW), jnp.maximum(one, two)

    per_a, per_b = row_ref.shape[1] // LANES, column_ref.shape[1] // LANES
    for k in range(rows // LANES):
        part = slice(k * LANES, (k + 1) * LANES)
        one = jnp.sum(row_one[part, :].T, axis=0, keepdims=True)
        two = jnp.sum(row_two[part, :].T, axis=0, keepdims=True)
        value, least = pick(one, two)
        worst = jnp.minimum(worst, least)
        q, r = k // per_a, k % per_a
        row_ref[q : q + 1, r * LANES : (r + 1) * LANES] = value
    for k in range(columns // LANES):
        part = slice(k * LANES, (k + 1) * LANES)
        one = jnp.sum(column_one[:, part], axis=0, keepdims=True)
        two = jnp.sum(column_two[:, part], axis=0, keepdims=True)
        value, least = pick(one, two)
        worst = jnp.minimum(worst, least)
        q, r = k // per_b, k % per_b
        column_ref[q : q + 1, r * LANES : (r + 1) * LANES] = value

    @pl.when(jnp.min(worst) < FLOOR)
    def exact():
        row_top, row_sum, column_top, column_sum = row_one, row_two, column_one, column_two
        least = jnp.finfo(jnp.float32).min
        row_top[...] = jnp.full_like(row_top, least)
        column_top[...] = jnp.full_like(column_top, least)
        row_sum[...] = jnp.zeros_like(row_sum)
        column_sum[...] = jnp.zeros_like(column_sum)
        low = tile(rows, 128)

        def walk(step):
            def over(k, carry):
                r = pl.ds(pl.multiple_of(lax.rem(k, rows // low) * low, low), low)
                c = pl.ds(pl.multiple_of(lax.div(k, rows // low) * wide, wide), wide)
                step(r, c, jnp.dot(at[r, :], bt[:, c], preferred_element_type=jnp.float32))
                return carry

            lax.fori_loop(0, (rows // low) * (columns // wide), over, 0)

        def tops(r, c, x):
            row_top[r, :] = jnp.maximum(row_top[r, :], lanes_of(x, jnp.maximum))
            column_top[:, c] = jnp.maximum(column_top[:, c], sublanes_of(x, jnp.maximum))

        def sums(r, c, x):
            e = jnp.exp2(x - jnp.concatenate([row_top[r, :]] * (wide // LANES), axis=1))
            row_sum[r, :] = row_sum[r, :] + lanes_of(e, jnp.add)
            e = jnp.exp2(x - jnp.concatenate([column_top[:, c]] * (low // 8), axis=0))
            column_sum[:, c] = column_sum[:, c] + sublanes_of(e, jnp.add)

        walk(tops)
        row_top[...] = jnp.broadcast_to(jnp.max(row_top[...], axis=1, keepdims=True), row_top.shape)
        column_top[...] = jnp.broadcast_to(jnp.max(column_top[...], axis=0, keepdims=True), column_top.shape)
        walk(sums)
        for k in range(rows // LANES):
            part = slice(k * LANES, (k + 1) * LANES)
            mass = jnp.sum(row_sum[part, :].T, axis=0, keepdims=True)
            q, r = k // per_a, k % per_a
            row_ref[q : q + 1, r * LANES : (r + 1) * LANES] = row_top[part, :].T[:1] + (jnp.log2(mass) + HIGH)
        for k in range(columns // LANES):
            part = slice(k * LANES, (k + 1) * LANES)
            mass = jnp.sum(column_sum[:, part], axis=0, keepdims=True)
            q, r = k // per_b, k % per_b
            column_ref[q : q + 1, r * LANES : (r + 1) * LANES] = column_top[:1, part] + (jnp.log2(mass) + HIGH)


def stats(a_parts, b_parts, place_a, place_b, moved, scale):
    tokens = a_parts[0].shape[0]
    rows, columns = (sum(part.shape[1] for part in parts) for parts in (a_parts, b_parts))
    blocks_a, blocks_b = (sum(len(p) for p in place) for place in (place_a, place_b))
    depth = round_up(3 * tokens + 1, LANES)
    vmem = pl.BlockSpec(memory_space=pltpu.VMEM)
    return pl.pallas_call(
        functools.partial(stats_kernel, scale, place_a, place_b, moved),
        out_shape=(
            jax.ShapeDtypeStruct((blocks_a, rows // blocks_a), jnp.float32),
            jax.ShapeDtypeStruct((blocks_b, columns // blocks_b), jnp.float32),
            jax.ShapeDtypeStruct((tokens, rows), jnp.bfloat16),
            jax.ShapeDtypeStruct((tokens, columns), jnp.bfloat16),
        ),
        in_specs=[vmem] * (len(a_parts) + len(b_parts)),
        out_specs=[vmem] * 4,
        scratch_shapes=[
            pltpu.VMEM((rows, depth), jnp.bfloat16),
            pltpu.VMEM((depth, columns), jnp.bfloat16),
            pltpu.VMEM((rows, LANES), jnp.float32),
            pltpu.VMEM((rows, LANES), jnp.float32),
            pltpu.VMEM((8, columns), jnp.float32),
            pltpu.VMEM((8, columns), jnp.float32),
        ],
        cost_estimate=pl.CostEstimate(
            flops=2 * rows * columns * depth, bytes_accessed=0, transcendentals=2 * rows * columns
        ),
        compiler_params=pltpu.CompilerParams(vmem_limit_bytes=32 * 2**20),
        name="stats",
    )(*a_parts, *b_parts)


def joined(parts):
    top = parts[0]
    for part in parts[1:]:
        top = jnp.maximum(top, part)
    mass = jnp.exp2(parts[0] - top)
    for part in parts[1:]:
        mass = mass + jnp.exp2(part - top)
    return top + jnp.log2(mass)


def match_kernel(count_a, count_b, *refs):
    a_ref, b_ref = refs[:2]
    row_parts, refs = refs[2 : 2 + count_a], refs[2 + count_a :]
    column_parts, refs = refs[:count_b], refs[count_b:]
    out_ref, row_level, column_level, at, bt, buffer, done = refs
    tokens, rows = a_ref.shape
    columns = b_ref.shape[1]
    slots, tall, _ = buffer.shape
    depth = at.shape[0]

    def finish(parts, target, level_ref):
        level = joined([part[...] for part in parts]) * (1.0 / (LOG2E * INV_TEMP))
        width = level.shape[1]
        for q in range(level.shape[0]):
            line = level[q : q + 1]
            for k in range(width // LANES):
                spot = q * (width // LANES) + k
                level_ref[spot : spot + 1, :] = line[:, k * LANES : (k + 1) * LANES]
            target(q * width, width, three(line * (-0.5 * tokens)))

    rest = depth - tokens - 6

    def row_terms(first, width, terms):
        one = jnp.ones((3, width), jnp.float32)
        lines = [term.astype(jnp.float32) for term in terms]
        at[tokens:, first : first + width] = jnp.concatenate(
            lines + [one, jnp.zeros((rest, width), jnp.float32)], axis=0
        ).astype(jnp.bfloat16)

    def column_terms(first, width, terms):
        one = jnp.ones((3, width), jnp.float32)
        lines = [term.astype(jnp.float32) for term in terms]
        bt[tokens:, first : first + width] = jnp.concatenate(
            [one] + lines + [jnp.zeros((rest, width), jnp.float32)], axis=0
        ).astype(jnp.bfloat16)

    at[:tokens, :] = a_ref[...]
    bt[:tokens, :] = b_ref[...]
    finish(row_parts, row_terms, row_level)
    finish(column_parts, column_terms, column_level)

    wide = tile(columns, 512)
    tiles = rows // tall

    def copy(t):
        slot = lax.rem(t, slots)
        where = pl.ds(pl.multiple_of(t * tall, tall), tall)
        return pltpu.make_async_copy(buffer.at[slot], out_ref.at[where], done.at[slot])

    def step(t, carry):
        slot = lax.rem(t, slots)

        @pl.when(t >= slots)
        def _():
            copy(t - slots).wait()

        left = at[:, pl.ds(pl.multiple_of(t * tall, tall), tall)].T
        for k in range(columns // wide):
            part = slice(k * wide, (k + 1) * wide)
            dots = jnp.dot(left, bt[:, part], preferred_element_type=jnp.float32)
            buffer[slot, :, part] = dots * (1.0 / tokens)
        copy(t).start()
        return carry

    lax.fori_loop(0, tiles, step, 0)
    for t in range(max(tiles - slots, 0), tiles):
        copy(t).wait()


def match(a, b, row_parts, column_parts):
    tokens, rows = a.shape
    columns = b.shape[1]
    tall = tile(rows, LANES)
    slots = 4
    depth = round_up(tokens + 6, 16)
    vmem = pl.BlockSpec(memory_space=pltpu.VMEM)
    return pl.pallas_call(
        functools.partial(match_kernel, len(row_parts), len(column_parts)),
        out_shape=(
            jax.ShapeDtypeStruct((rows, columns), jnp.float32),
            jax.ShapeDtypeStruct((rows // LANES, LANES), jnp.float32),
            jax.ShapeDtypeStruct((columns // LANES, LANES), jnp.float32),
        ),
        in_specs=[vmem] * (2 + len(row_parts) + len(column_parts)),
        out_specs=(pl.BlockSpec(memory_space=pl.ANY), vmem, vmem),
        scratch_shapes=[
            pltpu.VMEM((depth, rows), jnp.bfloat16),
            pltpu.VMEM((depth, columns), jnp.bfloat16),
            pltpu.VMEM((slots, tall, columns), jnp.float32),
            pltpu.SemaphoreType.DMA((slots,)),
        ],
        cost_estimate=pl.CostEstimate(
            flops=2 * rows * columns * depth, bytes_accessed=4 * rows * columns, transcendentals=0
        ),
        compiler_params=pltpu.CompilerParams(vmem_limit_bytes=32 * 2**20),
        name="match",
    )(a, b, *row_parts, *column_parts)


def slabs_kernel(x_ref, out_ref):
    count, copies, _, depth = out_ref.shape
    for q in range(count):
        part = x_ref[:, q * depth : (q + 1) * depth]
        for c in range(copies):
            out_ref[q, c] = part


def slabs(x, count, copies):
    rows, depth = x.shape[0], x.shape[1] // count
    vmem = pl.BlockSpec(memory_space=pltpu.VMEM)
    return pl.pallas_call(
        slabs_kernel,
        out_shape=jax.ShapeDtypeStruct((count, copies, rows, depth), x.dtype),
        in_specs=[vmem],
        out_specs=vmem,
        compiler_params=pltpu.CompilerParams(vmem_limit_bytes=8 * 2**20),
        name="slabs",
    )(x)


def swap(value, axis, distance):
    size = lax.axis_size(axis)
    return lax.ppermute(value, axis, [(k, k ^ distance) for k in range(size)])


def block_of(value, axis, part, parts, distance):
    size = lax.axis_size(axis)
    width = value.shape[1] // size
    start = (lax.axis_index(axis) ^ distance) * width + part * (width // parts)
    return lax.dynamic_slice_in_dim(value, start, width // parts, axis=1)


def scatter_sum(value, axis, near, parts):
    size = lax.axis_size(axis)
    near = min(near, size)
    far = range(0, size, near)
    width = value.shape[1] // size
    if width % (parts * LANES):
        parts = 1
    first = []
    for part in range(parts):
        sent = [
            jnp.concatenate([block_of(value, axis, part, parts, d ^ k) for k in far], axis=1) for d in range(near)
        ]
        first.append([sent[0]] + [swap(sent[d], axis, d) for d in range(near - 1, 0, -1)])
    done = []
    for got in first:
        total = functools.reduce(jnp.add, got)
        rest = jnp.split(total, len(far), axis=1)
        done.append(functools.reduce(jnp.add, [rest[0]] + [swap(r, axis, k) for r, k in zip(rest[1:], far[1:])]))
    return jnp.concatenate(done, axis=1) if parts > 1 else done[0]


def everyone(value, axis, near):
    size = lax.axis_size(axis)
    near = min(near, size)
    mine = [value] + [swap(value, axis, k) for k in range(near, size, near)]
    mine = jnp.concatenate(mine, axis=1) if len(mine) > 1 else value
    return [mine] + [swap(mine, axis, d) for d in range(near - 1, 0, -1)]


def distances(axis, near):
    near = min(near, lax.axis_size(axis))
    return [0] + list(range(near - 1, 0, -1))


def in_order(parts, axis, near):
    size = lax.axis_size(axis)
    near = min(near, size)
    blocks = [None] * size
    for d, part in zip(distances(axis, near), parts):
        for k, block in enumerate(jnp.split(part, size // near, axis=1)):
            blocks[d ^ (near * k)] = block
    order = lax.axis_index(axis) ^ jnp.arange(size)
    stacked = jnp.take(jnp.stack(blocks), order, axis=0)
    return jnp.transpose(stacked, (1, 0, 2)).reshape(parts[0].shape[0], -1)


def all_joined(value, axis):
    distance = 1
    while distance < lax.axis_size(axis):
        value = joined([value, swap(value, axis, distance)])
        distance *= 2
    return value


def standardize(encoded, bias, axis):
    width = encoded.shape[1]
    bias = lax.dynamic_slice_in_dim(bias, lax.axis_index(axis) * width, width)
    fired = jnp.maximum(encoded + bias[None, :], 0.0)
    centered = fired - jnp.mean(fired, axis=0)[None, :]
    spread = jnp.mean(centered * centered, axis=0)
    return (centered * lax.rsqrt(spread + epsilon)[None, :]).astype(jnp.bfloat16)


def per_device_inner(residual_a, residual_b, encoder_a, bias_a, encoder_b, bias_b):
    size_a, size_b = lax.axis_size("aa"), lax.axis_size("ba")
    index_a = lax.axis_index("aa")
    both = ("aa", "ba")

    own, depth = residual_b.shape[0], residual_b.shape[1] // size_a
    sent = slabs(residual_b, size_a, size_b).reshape(-1, own, depth)
    columns_b = lax.all_to_all(sent, both, 0, 0, tiled=True).reshape(-1, depth)
    partial_b = jnp.dot(columns_b, encoder_b, preferred_element_type=jnp.float32)
    encoded_b = scatter_sum(partial_b, "aa", NEAR_B, 2)

    ratio = size_a // size_b
    assert ratio * size_b == size_a
    tokens_a = lax.all_gather(residual_a, "ba", axis=0, tiled=True)
    tokens = tokens_a.shape[0]
    tokens_a, bias_a, bias_b, _ = lax.optimization_barrier((tokens_a, bias_a, bias_b, partial_b))
    got = []
    for p in range(ratio):
        pairs = [
            ((ratio * j + (i + p) % ratio) * size_b + i // ratio, i * size_b + j)
            for i in range(size_a)
            for j in range(size_b)
        ]
        got.append(lax.ppermute(tokens_a, both, pairs))
    columns_a = [got[0]]
    if ratio > 1:
        turned = jnp.roll(jnp.stack(got), index_a % ratio, axis=0)
        columns_a = [turned[p] for p in range(ratio)]
    columns_a = jnp.concatenate(columns_a, axis=1)
    partial_a = jnp.dot(columns_a, encoder_a, preferred_element_type=jnp.float32)
    encoded_a = scatter_sum(partial_a, "ba", size_b, 1)

    every_a = everyone(standardize(encoded_a, bias_a, "ba"), "ba", size_b)
    every_b = everyone(standardize(encoded_b, bias_b, "aa"), "aa", NEAR_B)

    near = min(NEAR_B, size_a)
    place_a = [[d] for d in distances("ba", size_b)]
    place_b = [[d ^ k for k in range(0, size_a, near)] for d in distances("aa", near)]
    moved = True
    if (bias_a.shape[0] // size_b % LANES or bias_b.shape[0] // size_a % LANES):
        every_a, every_b = [in_order(every_a, "ba", size_b)], [in_order(every_b, "aa", near)]
        place_a, place_b = [[0]], [[0]]
        moved = False
    row_part, column_part, all_a, all_b = stats(every_a, every_b, place_a, place_b, moved, LOG2E * INV_TEMP / tokens)
    column_part = all_joined(column_part, "aa")
    row_part = all_joined(row_part, "ba")
    match_score, row_level, column_level = match(all_a, all_b, [row_part], [column_part])
    return (match_score, row_level.reshape(-1), column_level.reshape(-1))


def solution(mesh):
    return jax.shard_map(
        per_device_inner,
        mesh=mesh,
        in_specs=(
            P("ba", "aa"),
            P(("aa", "ba"), None),
            P("ba", "aa"),
            P("aa"),
            P("aa", "ba"),
            P("ba"),
        ),
        out_specs=(P("aa", "ba"), P("aa"), P("ba")),
        check_vma=False,
    )
```

```python
import functools
import math

import jax
import jax.numpy as jnp
from jax import lax
from jax.experimental import pallas as pl
from jax.experimental.pallas import tpu as pltpu
from jax.sharding import PartitionSpec as P


INV_TEMP = 256
LOG2E = math.log2(math.e)
LANES = 128

NEAR_B = 4

epsilon = 1e-05


HIGH, LOW = 260.0, 52.0
FLOOR = 2.0**-96


def tile(size, most):
    while size % most:
        most //= 2
    return most


def round_up(size, unit):
    return -(-size // unit) * unit


def lanes_of(values, combine):
    total = values[:, :LANES]
    for k in range(1, values.shape[1] // LANES):
        total = combine(total, values[:, k * LANES : (k + 1) * LANES])
    return total


def sublanes_of(values, combine):
    total = values[:8]
    for k in range(1, values.shape[0] // 8):
        total = combine(total, values[k * 8 : (k + 1) * 8])
    return total


def three(value):
    high = value.astype(jnp.bfloat16)
    rest = value - high.astype(jnp.float32)
    middle = rest.astype(jnp.bfloat16)
    low = (rest - middle.astype(jnp.float32)).astype(jnp.bfloat16)
    return [high, middle, low]


def stats_kernel(scale, place_a, place_b, moved, *refs):
    a_parts, refs = refs[: len(place_a)], refs[len(place_a) :]
    b_parts, refs = refs[: len(place_b)], refs[len(place_b) :]
    row_ref, column_ref, a_all, b_all, at, bt, row_one, row_two, column_one, column_two = refs
    tokens, rows = a_all.shape
    columns = b_all.shape[1]
    part_a, part_b = row_ref.shape[1], column_ref.shape[1]
    depth = at.shape[1]
    used = 3 * tokens
    index = [lax.axis_index("aa"), lax.axis_index("ba")] if moved else [0, 0]

    spot = lax.broadcasted_iota(jnp.int32, (rows, depth - used), 1) == 0
    at[:, used:] = jnp.where(spot, -HIGH, 0.0).astype(jnp.bfloat16)
    spot = lax.broadcasted_iota(jnp.int32, (depth - used, columns), 0) == 0
    bt[used:, :] = jnp.where(spot, 1.0, 0.0).astype(jnp.bfloat16)
    for part, places in zip(a_parts, place_a):
        for q, place in enumerate(places):
            first = lax.bitwise_xor(index[1], place) * part_a
            block = part[:, q * part_a : (q + 1) * part_a]
            a_all[:, pl.ds(pl.multiple_of(first, part_a), part_a)] = block
            terms = jnp.concatenate(three(block.astype(jnp.float32) * scale), axis=0)
            for k in range(part_a // LANES):
                here = pl.ds(pl.multiple_of(first + k * LANES, LANES), LANES)
                at[here, :used] = terms[:, k * LANES : (k + 1) * LANES].T
    for part, places in zip(b_parts, place_b):
        for q, place in enumerate(places):
            block = part[:, q * part_b : (q + 1) * part_b]
            here = pl.ds(pl.multiple_of(lax.bitwise_xor(index[0], place) * part_b, part_b), part_b)
            b_all[:, here] = block
            for k in range(3):
                bt[k * tokens : (k + 1) * tokens, here] = block

    wide = tile(columns, 512)
    tall = tile(rows, 512)
    row_one[...] = jnp.zeros_like(row_one)
    row_two[...] = jnp.zeros_like(row_two)

    def over_columns(c, carry):
        here = pl.ds(pl.multiple_of(c * wide, wide), wide)
        one = jnp.zeros((8, wide), jnp.float32)
        two = one
        for k in range(rows // tall):
            band = slice(k * tall, (k + 1) * tall)
            x = jnp.dot(at[band, :], bt[:, here], preferred_element_type=jnp.float32)
            e = jnp.exp2(x)
            row_one[band, :] = row_one[band, :] + lanes_of(e, jnp.add)
            one = one + sublanes_of(e, jnp.add)
            e = jnp.exp2(x + (HIGH - LOW))
            row_two[band, :] = row_two[band, :] + lanes_of(e, jnp.add)
            two = two + sublanes_of(e, jnp.add)
        column_one[:, here] = one
        column_two[:, here] = two
        return carry

    lax.fori_loop(0, columns // wide, over_columns, 0)

    worst = jnp.full((1, LANES), jnp.inf, jnp.float32)

    def pick(one, two):
        return jnp.where(one >= FLOOR, jnp.log2(one) + HIGH, jnp.log2(two) + LOW), jnp.maximum(one, two)

    per_a, per_b = row_ref.shape[1] // LANES, column_ref.shape[1] // LANES
    for k in range(rows // LANES):
        part = slice(k * LANES, (k + 1) * LANES)
        one = jnp.sum(row_one[part, :].T, axis=0, keepdims=True)
        two = jnp.sum(row_two[part, :].T, axis=0, keepdims=True)
        value, least = pick(one, two)
        worst = jnp.minimum(worst, least)
        q, r = k // per_a, k % per_a
        row_ref[q : q + 1, r * LANES : (r + 1) * LANES] = value
    for k in range(columns // LANES):
        part = slice(k * LANES, (k + 1) * LANES)
        one = jnp.sum(column_one[:, part], axis=0, keepdims=True)
        two = jnp.sum(column_two[:, part], axis=0, keepdims=True)
        value, least = pick(one, two)
        worst = jnp.minimum(worst, least)
        q, r = k // per_b, k % per_b
        column_ref[q : q + 1, r * LANES : (r + 1) * LANES] = value

    @pl.when(jnp.min(worst) < FLOOR)
    def exact():
        row_top, row_sum, column_top, column_sum = row_one, row_two, column_one, column_two
        least = jnp.finfo(jnp.float32).min
        row_top[...] = jnp.full_like(row_top, least)
        column_top[...] = jnp.full_like(column_top, least)
        row_sum[...] = jnp.zeros_like(row_sum)
        column_sum[...] = jnp.zeros_like(column_sum)
        low = tile(rows, 128)

        def walk(step):
            def over(k, carry):
                r = pl.ds(pl.multiple_of(lax.rem(k, rows // low) * low, low), low)
                c = pl.ds(pl.multiple_of(lax.div(k, rows // low) * wide, wide), wide)
                step(r, c, jnp.dot(at[r, :], bt[:, c], preferred_element_type=jnp.float32))
                return carry

            lax.fori_loop(0, (rows // low) * (columns // wide), over, 0)

        def tops(r, c, x):
            row_top[r, :] = jnp.maximum(row_top[r, :], lanes_of(x, jnp.maximum))
            column_top[:, c] = jnp.maximum(column_top[:, c], sublanes_of(x, jnp.maximum))

        def sums(r, c, x):
            e = jnp.exp2(x - jnp.concatenate([row_top[r, :]] * (wide // LANES), axis=1))
            row_sum[r, :] = row_sum[r, :] + lanes_of(e, jnp.add)
            e = jnp.exp2(x - jnp.concatenate([column_top[:, c]] * (low // 8), axis=0))
            column_sum[:, c] = column_sum[:, c] + sublanes_of(e, jnp.add)

        walk(tops)
        row_top[...] = jnp.broadcast_to(jnp.max(row_top[...], axis=1, keepdims=True), row_top.shape)
        column_top[...] = jnp.broadcast_to(jnp.max(column_top[...], axis=0, keepdims=True), column_top.shape)
        walk(sums)
        for k in range(rows // LANES):
            part = slice(k * LANES, (k + 1) * LANES)
            mass = jnp.sum(row_sum[part, :].T, axis=0, keepdims=True)
            q, r = k // per_a, k % per_a
            row_ref[q : q + 1, r * LANES : (r + 1) * LANES] = row_top[part, :].T[:1] + (jnp.log2(mass) + HIGH)
        for k in range(columns // LANES):
            part = slice(k * LANES, (k + 1) * LANES)
            mass = jnp.sum(column_sum[:, part], axis=0, keepdims=True)
            q, r = k // per_b, k % per_b
            column_ref[q : q + 1, r * LANES : (r + 1) * LANES] = column_top[:1, part] + (jnp.log2(mass) + HIGH)


def stats(a_parts, b_parts, place_a, place_b, moved, scale):
    tokens = a_parts[0].shape[0]
    rows, columns = (sum(part.shape[1] for part in parts) for parts in (a_parts, b_parts))
    blocks_a, blocks_b = (sum(len(p) for p in place) for place in (place_a, place_b))
    depth = round_up(3 * tokens + 1, LANES)
    vmem = pl.BlockSpec(memory_space=pltpu.VMEM)
    return pl.pallas_call(
        functools.partial(stats_kernel, scale, place_a, place_b, moved),
        out_shape=(
            jax.ShapeDtypeStruct((blocks_a, rows // blocks_a), jnp.float32),
            jax.ShapeDtypeStruct((blocks_b, columns // blocks_b), jnp.float32),
            jax.ShapeDtypeStruct((tokens, rows), jnp.bfloat16),
            jax.ShapeDtypeStruct((tokens, columns), jnp.bfloat16),
        ),
        in_specs=[vmem] * (len(a_parts) + len(b_parts)),
        out_specs=[vmem] * 4,
        scratch_shapes=[
            pltpu.VMEM((rows, depth), jnp.bfloat16),
            pltpu.VMEM((depth, columns), jnp.bfloat16),
            pltpu.VMEM((rows, LANES), jnp.float32),
            pltpu.VMEM((rows, LANES), jnp.float32),
            pltpu.VMEM((8, columns), jnp.float32),
            pltpu.VMEM((8, columns), jnp.float32),
        ],
        cost_estimate=pl.CostEstimate(
            flops=2 * rows * columns * depth, bytes_accessed=0, transcendentals=2 * rows * columns
        ),
        compiler_params=pltpu.CompilerParams(vmem_limit_bytes=32 * 2**20),
        name="stats",
    )(*a_parts, *b_parts)


def joined(parts):
    top = parts[0]
    for part in parts[1:]:
        top = jnp.maximum(top, part)
    mass = jnp.exp2(parts[0] - top)
    for part in parts[1:]:
        mass = mass + jnp.exp2(part - top)
    return top + jnp.log2(mass)


def match_kernel(count_a, count_b, *refs):
    a_ref, b_ref = refs[:2]
    row_parts, refs = refs[2 : 2 + count_a], refs[2 + count_a :]
    column_parts, refs = refs[:count_b], refs[count_b:]
    out_ref, row_level, column_level, at, bt, buffer, done = refs
    tokens, rows = a_ref.shape
    columns = b_ref.shape[1]
    slots, tall, _ = buffer.shape
    depth = at.shape[0]

    def finish(parts, target, level_ref):
        level = joined([part[...] for part in parts]) * (1.0 / (LOG2E * INV_TEMP))
        width = level.shape[1]
        for q in range(level.shape[0]):
            line = level[q : q + 1]
            for k in range(width // LANES):
                spot = q * (width // LANES) + k
                level_ref[spot : spot + 1, :] = line[:, k * LANES : (k + 1) * LANES]
            target(q * width, width, three(line * (-0.5 * tokens)))

    rest = depth - tokens - 6

    def row_terms(first, width, terms):
        one = jnp.ones((3, width), jnp.float32)
        lines = [term.astype(jnp.float32) for term in terms]
        at[tokens:, first : first + width] = jnp.concatenate(
            lines + [one, jnp.zeros((rest, width), jnp.float32)], axis=0
        ).astype(jnp.bfloat16)

    def column_terms(first, width, terms):
        one = jnp.ones((3, width), jnp.float32)
        lines = [term.astype(jnp.float32) for term in terms]
        bt[tokens:, first : first + width] = jnp.concatenate(
            [one] + lines + [jnp.zeros((rest, width), jnp.float32)], axis=0
        ).astype(jnp.bfloat16)

    at[:tokens, :] = a_ref[...]
    bt[:tokens, :] = b_ref[...]
    finish(row_parts, row_terms, row_level)
    finish(column_parts, column_terms, column_level)

    wide = tile(columns, 512)
    tiles = rows // tall

    def copy(t):
        slot = lax.rem(t, slots)
        where = pl.ds(pl.multiple_of(t * tall, tall), tall)
        return pltpu.make_async_copy(buffer.at[slot], out_ref.at[where], done.at[slot])

    def step(t, carry):
        slot = lax.rem(t, slots)

        @pl.when(t >= slots)
        def _():
            copy(t - slots).wait()

        left = at[:, pl.ds(pl.multiple_of(t * tall, tall), tall)].T
        for k in range(columns // wide):
            part = slice(k * wide, (k + 1) * wide)
            dots = jnp.dot(left, bt[:, part], preferred_element_type=jnp.float32)
            buffer[slot, :, part] = dots * (1.0 / tokens)
        copy(t).start()
        return carry

    lax.fori_loop(0, tiles, step, 0)
    for t in range(max(tiles - slots, 0), tiles):
        copy(t).wait()


def match(a, b, row_parts, column_parts):
    tokens, rows = a.shape
    columns = b.shape[1]
    tall = tile(rows, LANES)
    slots = 4
    depth = round_up(tokens + 6, 16)
    vmem = pl.BlockSpec(memory_space=pltpu.VMEM)
    return pl.pallas_call(
        functools.partial(match_kernel, len(row_parts), len(column_parts)),
        out_shape=(
            jax.ShapeDtypeStruct((rows, columns), jnp.float32),
            jax.ShapeDtypeStruct((rows // LANES, LANES), jnp.float32),
            jax.ShapeDtypeStruct((columns // LANES, LANES), jnp.float32),
        ),
        in_specs=[vmem] * (2 + len(row_parts) + len(column_parts)),
        out_specs=(pl.BlockSpec(memory_space=pl.ANY), vmem, vmem),
        scratch_shapes=[
            pltpu.VMEM((depth, rows), jnp.bfloat16),
            pltpu.VMEM((depth, columns), jnp.bfloat16),
            pltpu.VMEM((slots, tall, columns), jnp.float32),
            pltpu.SemaphoreType.DMA((slots,)),
        ],
        cost_estimate=pl.CostEstimate(
            flops=2 * rows * columns * depth, bytes_accessed=4 * rows * columns, transcendentals=0
        ),
        compiler_params=pltpu.CompilerParams(vmem_limit_bytes=32 * 2**20),
        name="match",
    )(a, b, *row_parts, *column_parts)


def slabs_kernel(x_ref, out_ref):
    count, copies, _, depth = out_ref.shape
    for q in range(count):
        part = x_ref[:, q * depth : (q + 1) * depth]
        for c in range(copies):
            out_ref[q, c] = part


def slabs(x, count, copies):
    rows, depth = x.shape[0], x.shape[1] // count
    vmem = pl.BlockSpec(memory_space=pltpu.VMEM)
    return pl.pallas_call(
        slabs_kernel,
        out_shape=jax.ShapeDtypeStruct((count, copies, rows, depth), x.dtype),
        in_specs=[vmem],
        out_specs=vmem,
        compiler_params=pltpu.CompilerParams(vmem_limit_bytes=8 * 2**20),
        name="slabs",
    )(x)


def swap(value, axis, distance):
    size = lax.axis_size(axis)
    return lax.ppermute(value, axis, [(k, k ^ distance) for k in range(size)])


def block_of(value, axis, part, parts, distance):
    size = lax.axis_size(axis)
    width = value.shape[1] // size
    start = (lax.axis_index(axis) ^ distance) * width + part * (width // parts)
    return lax.dynamic_slice_in_dim(value, start, width // parts, axis=1)


def products(xs, encoder, axis, near, parts):
    size = lax.axis_size(axis)
    near = min(near, size)
    far = range(0, size, near)
    if encoder.shape[1] // size % (parts * LANES):
        parts = 1
    if len(xs) > 1:
        turned = jnp.roll(jnp.stack(xs), lax.axis_index("aa") % len(xs), axis=0)
        xs = [turned[p] for p in range(len(xs))]
    value = jnp.dot(jnp.concatenate(xs, axis=1), encoder, preferred_element_type=jnp.float32)
    return [
        [jnp.concatenate([block_of(value, axis, part, parts, d ^ k) for k in far], axis=1) for d in range(near)]
        for part in range(parts)
    ]


def scatter_sum(sent, axis, near):
    size = lax.axis_size(axis)
    near = min(near, size)
    far = range(0, size, near)
    first = []
    for blocks in sent:
        first.append([blocks[0]] + [swap(blocks[d], axis, d) for d in range(1, near)])
    done = []
    for got in first:
        rest = jnp.split(functools.reduce(jnp.add, got), len(far), axis=1)
        rest[1:] = [swap(r, axis, k) for r, k in zip(rest[1:], far[1:])]
        done.append(functools.reduce(jnp.add, rest))
    return jnp.concatenate(done, axis=1) if len(done) > 1 else done[0]


def everyone(value, axis, near):
    size = lax.axis_size(axis)
    near = min(near, size)
    mine = [value] + [swap(value, axis, k) for k in range(near, size, near)]
    mine = jnp.concatenate(mine, axis=1) if len(mine) > 1 else value
    return [mine] + [swap(mine, axis, d) for d in range(near - 1, 0, -1)]


def distances(axis, near):
    near = min(near, lax.axis_size(axis))
    return [0] + list(range(near - 1, 0, -1))


def in_order(parts, axis, near):
    size = lax.axis_size(axis)
    near = min(near, size)
    blocks = [None] * size
    for d, part in zip(distances(axis, near), parts):
        for k, block in enumerate(jnp.split(part, size // near, axis=1)):
            blocks[d ^ (near * k)] = block
    order = lax.axis_index(axis) ^ jnp.arange(size)
    stacked = jnp.take(jnp.stack(blocks), order, axis=0)
    return jnp.transpose(stacked, (1, 0, 2)).reshape(parts[0].shape[0], -1)


def all_joined(value, axis):
    distance = 1
    while distance < lax.axis_size(axis):
        value = joined([value, swap(value, axis, distance)])
        distance *= 2
    return value


def standardize(encoded, bias, axis):
    width = encoded.shape[1]
    bias = lax.dynamic_slice_in_dim(bias, lax.axis_index(axis) * width, width)
    fired = jnp.maximum(encoded + bias[None, :], 0.0)
    centered = fired - jnp.mean(fired, axis=0)[None, :]
    spread = jnp.mean(centered * centered, axis=0)
    return (centered * lax.rsqrt(spread + epsilon)[None, :]).astype(jnp.bfloat16)


def per_device_inner(residual_a, residual_b, encoder_a, bias_a, encoder_b, bias_b):
    size_a, size_b = lax.axis_size("aa"), lax.axis_size("ba")
    both = ("aa", "ba")

    own, depth = residual_b.shape[0], residual_b.shape[1] // size_a
    sent = slabs(residual_b, size_a, size_b).reshape(-1, own, depth)
    columns_b = lax.all_to_all(sent, both, 0, 0, tiled=True)
    columns_b = columns_b.reshape(-1, depth)
    sent_b = products([columns_b], encoder_b, "aa", NEAR_B, 2)
    encoded_b = scatter_sum(sent_b, "aa", NEAR_B)

    ratio = size_a // size_b
    assert ratio * size_b == size_a
    tokens_a = lax.all_gather(residual_a, "ba", axis=0, tiled=True)
    tokens = tokens_a.shape[0]
    tokens_a, bias_a, bias_b, _ = lax.optimization_barrier((tokens_a, bias_a, bias_b, sent_b[0][0]))
    got = []
    for p in range(ratio):
        pairs = [
            ((ratio * j + (i + p) % ratio) * size_b + i // ratio, i * size_b + j)
            for i in range(size_a)
            for j in range(size_b)
        ]
        got.append(lax.ppermute(tokens_a, both, pairs))
    sent_a = products(got, encoder_a, "ba", size_b, 1)
    encoded_a = scatter_sum(sent_a, "ba", size_b)

    every_a = everyone(standardize(encoded_a, bias_a, "ba"), "ba", size_b)
    every_b = everyone(standardize(encoded_b, bias_b, "aa"), "aa", NEAR_B)

    near = min(NEAR_B, size_a)
    place_a = [[d] for d in distances("ba", size_b)]
    place_b = [[d ^ k for k in range(0, size_a, near)] for d in distances("aa", near)]
    moved = True
    if (bias_a.shape[0] // size_b % LANES or bias_b.shape[0] // size_a % LANES):
        every_a, every_b = [in_order(every_a, "ba", size_b)], [in_order(every_b, "aa", near)]
        place_a, place_b = [[0]], [[0]]
        moved = False
    row_part, column_part, all_a, all_b = stats(every_a, every_b, place_a, place_b, moved, LOG2E * INV_TEMP / tokens)
    column_part = all_joined(column_part, "aa")
    row_part = all_joined(row_part, "ba")
    match_score, row_level, column_level = match(all_a, all_b, [row_part], [column_part])
    return (match_score, row_level.reshape(-1), column_level.reshape(-1))


def solution(mesh):
    return jax.shard_map(
        per_device_inner,
        mesh=mesh,
        in_specs=(
            P("ba", "aa"),
            P(("aa", "ba"), None),
            P("ba", "aa"),
            P("aa"),
            P("aa", "ba"),
            P("ba"),
        ),
        out_specs=(P("aa", "ba"), P("aa"), P("ba")),
        check_vma=False,
    )
```
